256 devices in a mesh: groups: 2 (over z), owner: 128 (over y, x, core).
Axes of the slice: x: 8, y: 8, z: 2, core: 2. Of those that a mesh axis runs over, the one named last changes fastest.
The devices are a block of a 8x8x16 slice.
Arguments:
- queries: bfloat16 [16384, 1024], P(('groups', 'owner')), parts along dimension 0, may hold values from -0.3984375 to 0.3984375
- probes: int32 [16384, 8], P(('groups', 'owner')), parts along dimension 0, may hold values from 0 to 2047, as said below
- passages: bfloat16 [2048, 256, 1024], P('owner'), may hold values from -6 to 6
- centroids: bfloat16 [2048, 1024], P('owner'), may hold values from -6 to 6
- counts: int32 [2048], P('owner'), may hold values from 1 to 256
Outputs:
- scores: float32 [16384, 8, 256], P(('groups', 'owner')), parts along dimension 0
- visits: int32 [16384], P(('groups', 'owner')), parts along dimension 0
The draws below stay inside these ranges and needn't reach their ends.
There are 2 independent parts, one for each index of `groups`. The reference program is written for one: setup_inputs(seed, part) draws one part's arguments, and reference() takes and returns one part's arrays. A program takes and returns all parts, laid end to end along the dimension named above; an argument that names none is the same for every part. Nothing has to cross between parts.
Inputs may be any that keep to these rules, and one draw needn't show every extreme that they name: Cluster c belongs to owner index c // 16. In each aligned block of 64 queries (the queries of one index of owner) at most 8 probes name clusters of one owner, and in every draw some owners receive exactly 8 probes from every block. A query may name a cluster more than once.
All inputs are finite; a program needn't handle non-finite values.
Results may differ from the reference program's by a relative error of at most 0.0003.
Values may be sent and summed in bfloat16 or wider, within the bound.
A program may use at most 64 MiB of HBM per device.

```python
import jax
import jax.numpy as jnp
from jax import lax

D = 1024
PASSAGES = 256
PROBES = 8
Q_DEV = 64
CL_DEV = 16
QUERIES = 8192
CLUSTERS = 2048
CAP = 8


def draw_probes(key, part):
    owner_total = CLUSTERS // CL_DEV
    slot_total = owner_total * CAP
    pick_total = Q_DEV * PROBES
    hot_key, rest_key = jax.random.split(jax.random.fold_in(key, 17))
    shuffled = jax.random.permutation(hot_key, owner_total)
    hotness = (shuffled < owner_total // 8).astype(jnp.int32)
    source_keys = jax.random.split(rest_key, owner_total)

    def one_source(source_key):
        key_prio, key_order, key_local = jax.random.split(source_key, 3)
        positions = jnp.arange(slot_total, dtype=jnp.int32)
        slot_owner = positions // CAP
        priority = jax.random.randint(key_prio, (slot_total,), 0, 1024) + hotness[slot_owner] * 2048
        priority = priority * slot_total + positions
        unused, chosen = lax.top_k(priority, pick_total)
        chosen = jax.random.permutation(key_order, chosen)
        local_ids = jax.random.randint(key_local, (pick_total,), 0, CL_DEV)
        return (chosen // CAP * CL_DEV + local_ids).astype(jnp.int32).reshape(Q_DEV, PROBES)
    return jax.vmap(one_source)(source_keys).reshape(QUERIES, PROBES)


def plant(values, stream_key, least, top_value):
    longest = values.shape.index(max(values.shape))
    spots = []
    for shift in (0, 1):
        where = [jax.random.randint(jax.random.fold_in(stream_key, axis), (), 0, length) for axis, length in enumerate(values.shape)]
        where[longest] = (where[longest] + shift) % values.shape[longest]
        spots.append(tuple(where))
    return values.at[spots[0]].set(least).at[spots[1]].set(top_value)


def steps_of(rng, extent, shards, smallest, high):
    factor_of, own = 1.0, jax.random.fold_in(rng, 6)
    for position, blocks in shards:
        steps = jnp.exp(jax.random.uniform(jax.random.fold_in(own, position), (blocks,), jnp.float32, smallest / len(shards), high / len(shards)))
        factor_of = factor_of * jnp.repeat(steps, extent[position] // blocks).reshape([-1 if axis == position else 1 for axis in range(len(extent))])
    return factor_of


def bell_draw(stream_key, dims, scale, reach, shards=(), kind=jnp.bfloat16):
    drawn = scale * jax.random.normal(stream_key, dims, jnp.float32)
    if shards:
        drawn = drawn * steps_of(stream_key, dims, shards, -0.22, 0.18)
    return jnp.clip(drawn, -reach, reach).astype(kind)


def setup_inputs(seed: int = 0, part: int = 0) -> dict:
    key_of = jax.random.split(jax.random.key(seed), 6)
    part_splits = jax.random.split(jax.random.fold_in(key_of[5], part), 6)
    return {
        "queries": bell_draw(part_splits[0], (QUERIES, D), 0.05, 0.3984375, ((0, 128),)),
        "probes": draw_probes(jax.random.fold_in(jax.random.fold_in(key_of[5], part), 71), part),
        "passages": bell_draw(key_of[2], (CLUSTERS, PASSAGES, D), 1.0, 6.0, ((0, 128),)),
        "centroids": bell_draw(key_of[3], (CLUSTERS, D), 1.0, 6.0, ((0, 128),)),
        "counts": plant(jax.random.randint(key_of[4], (CLUSTERS,), 1, PASSAGES + 1), jax.random.fold_in(key_of[4], 1), 1, PASSAGES).astype(jnp.int32),
    }


def reference(queries, probes, passages, centroids, counts):
    query_count, probe_count = probes.shape
    pair_count = query_count * probe_count
    block_size = 256
    cluster_list = probes.reshape(pair_count // block_size, block_size).astype(jnp.int32)
    query_list = (jnp.arange(pair_count, dtype=jnp.int32) // probe_count).reshape(pair_count // block_size, block_size)

    def score_block(pieces):
        cluster_ids, query_ids = pieces
        query_rows = queries[query_ids].astype(jnp.float32)
        chosen = passages[cluster_ids].astype(jnp.float32)
        direct = jnp.einsum('bd,btd->bt', query_rows, chosen)
        centre = jnp.sum(query_rows * centroids[cluster_ids].astype(jnp.float32), axis=1)
        live_mask = jnp.arange(PASSAGES, dtype=jnp.int32)[None, :] < counts[cluster_ids][:, None]
        return jnp.where(live_mask, direct + centre[:, None], jnp.float32(0.0))

    scores = lax.map(score_block, (cluster_list, query_list)).reshape(query_count, probe_count, PASSAGES)
    visits = jnp.sum(counts[probes], axis=1).astype(jnp.int32)
    return scores, visits
```

```python
import functools
import math

import jax
import jax.numpy as jnp
from jax import lax
from jax.experimental import pallas as pl
from jax.experimental.pallas import tpu as pltpu
from jax.sharding import PartitionSpec as P

MESH = pl.DeviceIdType.MESH
LANES = 128
CODE_TOP = 32767.0


def iota(shape, dim):
    return lax.broadcasted_iota(jnp.int32, shape, dim)


def shift_of(t):
    return (2 * lax.rem(t, 2) - 1) * lax.div(t + 1, 2)


def kernel(
    side,
    cap,
    q_hbm,
    pcol_ref,
    pass_hbm,
    cent_ref,
    cnt_ref,
    out_ref,
    vis_ref,
    gq,
    gcode,
    snd,
    scid,
    rcv,
    rcid,
    acc,
    rs,
    sm,
    ret,
    rmeta,
    pv,
    tgt,
    slot_ref,
    load_sem,
    pass_sem,
    gq_send,
    gq_recv,
    gc_send,
    gc_recv,
    x_send,
    x_recv,
    c_send,
    c_recv,
    b_send,
    b_recv,
    m_send,
    m_recv,
):
    me = lax.axis_index("owner")
    core = lax.rem(me, 2)
    x = lax.rem(lax.div(me, 2), side)
    y = lax.div(me, 2 * side)
    local_count, span, width = pv.shape
    per_device = gq.shape[1]
    pair_count = pcol_ref.shape[0]
    probe_count = pair_count // per_device
    owner_count = side * side * 2
    pairs = side // 2
    dests = side * 2
    rows = dests * 2 * cap

    def wrap(v):
        return lax.rem(v + side, side)

    def device(first, second, cls, dest_core):
        yy = wrap(y + second * (1 - cls) + first * cls)
        xx = wrap(x + first * (1 - cls) + second * cls)
        return {"owner": (yy * side + xx) * 2 + dest_core}

    def remote(src, dst, send, recv, dev):
        return pltpu.make_async_remote_copy(
            src_ref=src, dst_ref=dst, send_sem=send, recv_sem=recv, device_id=dev, device_id_type=MESH
        )

    own_q = pltpu.make_async_copy(q_hbm, gq.at[0], load_sem)
    own_q.start()
    own_p = pltpu.make_async_copy(pass_hbm, pv, pass_sem)
    own_p.start()

    barrier = pltpu.get_barrier_semaphore()

    def greet(t, carry):
        for dest_core in range(2):
            for axis in range(2):
                pl.semaphore_signal(
                    barrier, inc=1, device_id=device(0, shift_of(t), axis, dest_core), device_id_type=MESH
                )
        return carry

    lax.fori_loop(1, side, greet, 0)
    pl.semaphore_signal(barrier, inc=1, device_id=device(0, 0, 0, 1 - core), device_id_type=MESH)

    pcol = pcol_ref[...]
    owner_col = lax.div(pcol, local_count)
    hits = (owner_col == iota((pair_count, owner_count), 1)).astype(jnp.float32)
    earlier = (iota((pair_count, pair_count), 0) > iota((pair_count, pair_count), 1)).astype(jnp.float32)
    before = jnp.dot(
        earlier.astype(jnp.bfloat16), hits.astype(jnp.bfloat16), preferred_element_type=jnp.float32
    )
    rank = jnp.sum(hits * before, axis=1, keepdims=True).astype(jnp.int32)
    slot_col = owner_col * cap + rank
    slot_ref[...] = slot_col
    code_col = slot_col * local_count + lax.rem(pcol, local_count)
    lane = iota((pair_count, LANES), 1)
    at_lane = lax.rem(lane, per_device) == lax.div(iota((pair_count, LANES), 0), probe_count)
    gcode[0] = jnp.sum(jnp.where(at_lane, code_col, 0).reshape(per_device, probe_count, LANES), axis=0)

    row = iota((rows, LANES), 0)
    dest = lax.div(row, 2 * cap)
    second = shift_of(lax.div(dest, 2))
    yy = wrap(y + second * (1 - core))
    xx = wrap(x + second * core)
    row_slot = ((yy * side + xx) * 2 + lax.rem(dest, 2)) * cap + lax.rem(row, cap)
    mine = lax.rem(lax.div(row, cap), 2) == lax.div(iota((rows, LANES), 1), per_device)
    tgt[...] = jnp.where(mine, row_slot, -1)

    own_q.wait()
    pl.semaphore_wait(barrier, 4 * (side - 1) + 1)

    def share(t, carry):
        dev = device(shift_of(t), 0, core, core)
        remote(gcode.at[0], gcode.at[t], gc_send.at[t], gc_recv.at[t], dev).start()
        remote(gq.at[0], gq.at[t], gq_send.at[t], gq_recv.at[t], dev).start()
        return carry

    lax.fori_loop(1, side, share, 0)

    def to_owner(p, f, dest_core):
        dev = device(0, shift_of(f), core, dest_core)
        d = f * 2 + dest_core
        return (
            remote(snd.at[p, d], rcv.at[p, f * 2 + core], x_send.at[p], x_recv.at[p], dev),
            remote(scid.at[p, d], rcid.at[p, f * 2 + core], c_send.at[p], c_recv.at[p], dev),
        )

    for p in range(pairs):
        for t in (2 * p, 2 * p + 1):
            if t:
                dev = device(0, 0, core, core)
                remote(gcode.at[0], gcode.at[t], gc_send.at[t], gc_recv.at[t], dev).wait_recv()
                remote(gq.at[0], gq.at[t], gq_send.at[t], gq_recv.at[t], dev).wait_recv()
        code = jnp.where(iota((probe_count, LANES), 1) < per_device, gcode[2 * p], gcode[2 * p + 1])
        slot_of = lax.div(code, local_count)
        mark_of = (lax.rem(code, local_count) + 1).astype(jnp.float32)
        target = tgt[...]
        mark = jnp.zeros((rows, LANES), jnp.float32)
        for j in range(probe_count):
            mark = jnp.where(target == slot_of[j : j + 1, :], mark_of[j : j + 1, :], mark)
        pick = jnp.where(mark > 0.0, 1.0, 0.0).astype(jnp.bfloat16)
        step = 256
        for n in range(0, width, step):
            part = gq[2 * p : 2 * p + 2, :, n : n + step].reshape(2 * per_device, step)
            took = jnp.dot(pick, part, preferred_element_type=jnp.float32)
            snd[p, :, :, n : n + step] = took.astype(jnp.bfloat16).reshape(dests, 2 * cap, step)
        mark_col = jnp.sum(mark, axis=1, keepdims=True)
        spot = iota((rows, LANES), 1) == lax.rem(iota((rows, LANES), 0), 2 * cap)
        marks = jnp.sum(jnp.where(spot, mark_col, 0.0).reshape(dests, 2 * cap, LANES), axis=1)
        for d in range(dests):
            scid[p, d] = marks[d : d + 1, :]

        self_x = pltpu.make_async_copy(snd.at[p, core], rcv.at[p, core], x_recv.at[p])
        self_c = pltpu.make_async_copy(scid.at[p, core], rcid.at[p, core], c_recv.at[p])
        self_c.start()
        self_x.start()
        for copy in to_owner(p, 0, 1 - core):
            copy.start()

        def post(f, carry):
            for dest_core in range(2):
                a, b = to_owner(p, f, dest_core)
                b.start()
                a.start()
            return carry

        lax.fori_loop(1, side, post, 0)

    def whole(ref, sem):
        return pltpu.make_async_copy(ref, ref, sem)

    own_p.wait()

    def back(p, f, cls, i):
        t = 2 * p + i
        dev = device(-shift_of(t), -shift_of(f), cls, cls)
        b = (f * 2 + cls) * 2 + i
        land = (f * 2 + core) * 2 + i
        return (
            remote(sm.at[p, b], rmeta.at[p, land], m_send.at[p], m_recv.at[p], dev),
            remote(rs.at[p, b], ret.at[p, land], b_send.at[p], b_recv.at[p], dev),
        )

    for p in range(pairs):
        whole(rcid.at[p], c_recv.at[p]).wait()
        whole(rcv.at[p], x_recv.at[p]).wait()
        row = iota((rows, LANES), 0)
        lane = iota((rows, LANES), 1)
        seen = jnp.broadcast_to(rcid[p], (dests, 2 * cap, LANES)).reshape(rows, LANES)
        cid = jnp.sum(jnp.where(lane == lax.rem(row, 2 * cap), seen, 0.0), axis=1, keepdims=True) - 1.0
        cid = cid.astype(jnp.int32)
        acc[...] = jnp.zeros_like(acc)

        def cluster(c, carry):
            got = lax.dot_general(
                rcv[p].reshape(rows, width),
                pv[c],
                (((1,), (1,)), ((), ())),
                preferred_element_type=jnp.float32,
            )
            acc[...] = jnp.where(cid == c, got, acc[...])
            return carry

        lax.fori_loop(0, local_count, cluster, 0)
        centres = lax.dot_general(
            rcv[p].reshape(rows, width),
            cent_ref[...],
            (((1,), (1,)), ((), ())),
            preferred_element_type=jnp.float32,
        )
        of_row = iota((rows, local_count), 1) == cid
        centre = jnp.sum(jnp.where(of_row, centres, 0.0), axis=1, keepdims=True)
        live = jnp.sum(jnp.where(of_row, cnt_ref[...], 0.0), axis=1, keepdims=True)
        within = iota((rows, span), 1).astype(jnp.float32) < live
        value = jnp.where(within, acc[...] + centre, 0.0)
        top = jnp.maximum(jnp.max(jnp.abs(value), axis=1, keepdims=True), 1e-30)
        coded = jnp.round(value * (CODE_TOP / top)).astype(jnp.int32)
        low, high = coded[:, : span // 2], coded[:, span // 2 :]
        rs[p] = (high * 65536 + (low & 65535)).reshape(dests * 2, cap, LANES)
        spot = lax.rem(lane, cap) == lax.rem(row, cap)
        scales = jnp.sum(
            jnp.where(spot, top * (1.0 / CODE_TOP), 0.0).reshape(dests * 2, cap, LANES), axis=1
        )
        lives = jnp.sum(jnp.where(spot, live, 0.0).reshape(dests * 2, cap, LANES), axis=1)
        both = jnp.concatenate([scales, lives], axis=1)
        for b in range(dests * 2):
            sm[p, b] = both[b : b + 1, :]

        def give(f, carry):
            for cls in range(2):
                for i in range(2):
                    for copy in back(p, f, cls, i):
                        copy.start()
            return carry

        if p == 0:
            self_b = core * 2
            pltpu.make_async_copy(sm.at[0, self_b], rmeta.at[0, self_b], m_recv.at[0]).start()
            pltpu.make_async_copy(rs.at[0, self_b], ret.at[0, self_b], b_recv.at[0]).start()
            for copy in back(0, 0, 1 - core, 0):
                copy.start()
            for cls in range(2):
                for copy in back(0, 0, cls, 1):
                    copy.start()
            lax.fori_loop(1, side, give, 0)
        else:
            lax.fori_loop(0, side, give, 0)

    scale_col = jnp.zeros((pair_count, 1), jnp.float32)
    live_col = jnp.zeros((pair_count, 1), jnp.float32)
    slots = slot_ref[...]
    for p in range(pairs):
        whole(rmeta.at[p], m_recv.at[p]).wait()
        whole(ret.at[p], b_recv.at[p]).wait()
        spot_lane = iota((1, rows), 1)
        block = lax.div(spot_lane, cap)
        second = shift_of(lax.div(block, 4))
        first = shift_of(2 * p + lax.rem(block, 2))
        yy = wrap(y + second * (1 - core) + first * core)
        xx = wrap(x + first * (1 - core) + second * core)
        have = ((yy * side + xx) * 2 + lax.rem(lax.div(block, 2), 2)) * cap + lax.rem(spot_lane, cap)
        match = slots == have
        pick = jnp.where(match, 1.0, 0.0).astype(jnp.bfloat16)
        words = ret[p].reshape(rows, LANES)

        def piece(low, high):
            return jnp.concatenate([low, high], axis=1).astype(jnp.float32).astype(jnp.bfloat16)

        tops = piece(
            lax.shift_right_arithmetic(lax.shift_left(words, 16), 24), lax.shift_right_arithmetic(words, 24)
        )
        tails = piece(words & 255, lax.shift_right_arithmetic(words, 16) & 255)
        sums = 256.0 * jnp.dot(pick, tops, preferred_element_type=jnp.float32) + jnp.dot(
            pick, tails, preferred_element_type=jnp.float32
        )
        out_ref[...] = sums if p == 0 else out_ref[...] + sums
        each = LANES // cap
        scale_lane, live_lane = [], []
        for h in range(rows // LANES):
            meta = jnp.concatenate([rmeta[p, h * each + b] for b in range(each)], axis=0)
            keep = lax.div(iota((each, LANES), 1), cap) == iota((each, LANES), 0)
            scale_lane.append(jnp.sum(jnp.where(keep, meta[:, :LANES], 0.0), axis=0, keepdims=True))
            live_lane.append(jnp.sum(jnp.where(keep, meta[:, LANES:], 0.0), axis=0, keepdims=True))
        scale_col += jnp.sum(
            jnp.where(match, jnp.concatenate(scale_lane, axis=1), 0.0), axis=1, keepdims=True
        )
        live_col += jnp.sum(jnp.where(match, jnp.concatenate(live_lane, axis=1), 0.0), axis=1, keepdims=True)
    out_ref[...] = out_ref[...] * scale_col
    at_query = iota((pair_count, LANES), 1) == lax.div(iota((pair_count, LANES), 0), probe_count)
    vis_ref[...] = jnp.sum(jnp.where(at_query, live_col, 0.0), axis=0, keepdims=True).astype(jnp.int32)

    def sent(t, carry):
        dev = device(shift_of(t), 0, core, core)
        remote(gcode.at[0], gcode.at[t], gc_send.at[t], gc_recv.at[t], dev).wait_send()
        remote(gq.at[0], gq.at[t], gq_send.at[t], gq_recv.at[t], dev).wait_send()
        return carry

    lax.fori_loop(1, side, sent, 0)
    for p in range(pairs):
        whole(snd.at[p, pl.ds(0, dests - 1)], x_send.at[p]).wait()
        whole(scid.at[p, pl.ds(0, dests - 1)], c_send.at[p]).wait()
        blocks = dests * 2 - (1 if p == 0 else 0)
        whole(rs.at[p, pl.ds(0, blocks)], b_send.at[p]).wait()
        whole(sm.at[p, pl.ds(0, blocks)], m_send.at[p]).wait()


def body(queries, probes, passages, centroids, counts):
    owner_count = lax.axis_size("owner")
    side = math.isqrt(owner_count // 2)
    per_device, probe_count = probes.shape
    local_count, span, width = passages.shape
    pair_count = per_device * probe_count
    cap = 2 * pair_count // owner_count
    pairs = side // 2
    dests = side * 2
    rows = dests * 2 * cap
    vmem = pl.BlockSpec(memory_space=pltpu.VMEM)
    hbm = pl.BlockSpec(memory_space=pl.ANY)
    dma = pltpu.SemaphoreType.DMA
    scores, visits = pl.pallas_call(
        functools.partial(kernel, side, cap),
        out_shape=(
            jax.ShapeDtypeStruct((pair_count, span), jnp.float32),
            jax.ShapeDtypeStruct((1, LANES), jnp.int32),
        ),
        in_specs=[hbm, vmem, hbm, vmem, vmem],
        out_specs=(vmem, vmem),
        scratch_shapes=[
            pltpu.VMEM((side, per_device, width), jnp.bfloat16),
            pltpu.VMEM((side, probe_count, LANES), jnp.int32),
            pltpu.VMEM((pairs, dests, 2 * cap, width), jnp.bfloat16),
            pltpu.VMEM((pairs, dests, 1, LANES), jnp.float32),
            pltpu.VMEM((pairs, dests, 2 * cap, width), jnp.bfloat16),
            pltpu.VMEM((pairs, dests, 1, LANES), jnp.float32),
            pltpu.VMEM((rows, span), jnp.float32),
            pltpu.VMEM((pairs, dests * 2, cap, LANES), jnp.int32),
            pltpu.VMEM((pairs, dests * 2, 1, 2 * LANES), jnp.float32),
            pltpu.VMEM((pairs, dests * 2, cap, LANES), jnp.int32),
            pltpu.VMEM((pairs, dests * 2, 1, 2 * LANES), jnp.float32),
            pltpu.VMEM((local_count, span, width), jnp.bfloat16),
            pltpu.VMEM((rows, LANES), jnp.int32),
            pltpu.VMEM((pair_count, 1), jnp.int32),
            dma,
            dma,
            dma((side,)),
            dma((side,)),
            dma((side,)),
            dma((side,)),
            dma((pairs,)),
            dma((pairs,)),
            dma((pairs,)),
            dma((pairs,)),
            dma((pairs,)),
            dma((pairs,)),
            dma((pairs,)),
            dma((pairs,)),
        ],
        compiler_params=pltpu.CompilerParams(
            collective_id=0, has_side_effects=True, vmem_limit_bytes=48 * 1024 * 1024
        ),
    )(
        queries,
        probes.reshape(pair_count, 1),
        passages,
        centroids,
        counts.astype(jnp.float32).reshape(1, local_count),
    )
    return scores.reshape(per_device, probe_count, span), visits[0, :per_device]


def solution(mesh):
    in_specs = (
        P(("groups", "owner"), None),
        P(("groups", "owner"), None),
        P("owner", None, None),
        P("owner", None),
        P("owner"),
    )
    out_specs = (P(("groups", "owner"), None, None), P(("groups", "owner")))
    return jax.shard_map(body, mesh=mesh, in_specs=in_specs, out_specs=out_specs, check_vma=False)
```

```python
import functools
import math

import jax
import jax.numpy as jnp
from jax import lax
from jax.experimental import pallas as pl
from jax.experimental.pallas import tpu as pltpu
from jax.sharding import PartitionSpec as P

MESH = pl.DeviceIdType.MESH
LANES = 128
CODE_TOP = 32767.0
ORDER = (
    "B0", "P", "B1", "B2", "X0", "S0", "B3", "X1", "S1", "G0", "X2", "S2",
    "G1", "X3", "G2", "S3", "G3", "F0", "F1", "F2", "F3",
)


def iota(shape, dim):
    return lax.broadcasted_iota(jnp.int32, shape, dim)


def shift_of(t):
    return (2 * lax.rem(t, 2) - 1) * lax.div(t + 1, 2)


def shift_int(t):
    return (t + 1) // 2 * (1 if t % 2 else -1)


def number_of(shift, side):
    return next(t for t in range(side) if (shift_int(t) - shift) % side == 0)


def kernel(
    side,
    cap,
    q_hbm,
    probe_hbm,
    pass_hbm,
    cent_hbm,
    cnt_hbm,
    out_ref,
    vis_ref,
    probe_ref,
    cent_ref,
    cnt_ref,
    gq,
    gcode,
    snd,
    scid,
    rcv,
    rcid,
    acc,
    rs,
    sm,
    ret,
    rmeta,
    pv,
    tgt,
    slot_ref,
    load_sem,
    small_sem,
    pass_sem,
    gq_send,
    gq_recv,
    gc_send,
    gc_recv,
    x_send,
    x_recv,
    c_send,
    c_recv,
    b_send,
    b_recv,
    m_send,
    m_recv,
):
    me = lax.axis_index("owner")
    core = lax.rem(me, 2)
    x = lax.rem(lax.div(me, 2), side)
    y = lax.div(me, 2 * side)
    local_count, span, width = pv.shape
    per_device = gq.shape[1]
    probe_count = probe_ref.shape[0]
    pair_count = per_device * probe_count
    owner_count = side * side * 2
    pairs = side // 2
    dests = side * 2
    rows = dests * 2 * cap

    def wrap(v):
        return lax.rem(v + side, side)

    ys = [wrap(y + shift_int(t)) * (2 * side) for t in range(side)]
    xs = [wrap(x + shift_int(t)) * 2 for t in range(side)]
    on_first = [(1 - core) * (ys[0] + xs[t]) + core * (ys[t] + xs[0]) for t in range(side)]
    on_second = [(1 - core) * (ys[t] + xs[0]) + core * (ys[0] + xs[t]) for t in range(side)]
    mirror = [number_of(-shift_int(t), side) for t in range(side)]

    def at(index):
        return {"owner": index}

    def remote(src, dst, send, recv, dev):
        return pltpu.make_async_remote_copy(
            src_ref=src, dst_ref=dst, send_sem=send, recv_sem=recv, device_id=dev, device_id_type=MESH
        )

    small = [
        pltpu.make_async_copy(src, dst, small_sem.at[n])
        for n, (src, dst) in enumerate(((probe_hbm, probe_ref), (cent_hbm, cent_ref), (cnt_hbm, cnt_ref)))
    ]
    for copy in small:
        copy.start()
    own_q = pltpu.make_async_copy(q_hbm, gq.at[0], load_sem)
    own_q.start()
    own_p = pltpu.make_async_copy(pass_hbm, pv, pass_sem)

    barrier = pltpu.get_barrier_semaphore()

    for t in range(1, side):
        for dest_core in range(2):
            for index in (ys[t] + xs[0], ys[0] + xs[t]):
                pl.semaphore_signal(barrier, inc=1, device_id=at(index + dest_core), device_id_type=MESH)
    partner = ys[0] + xs[0] + 1 - core
    pl.semaphore_signal(barrier, inc=1, device_id=at(partner), device_id_type=MESH)

    for copy in small:
        copy.wait()
    by_query = jnp.transpose(probe_ref[...].astype(jnp.float32))
    spread = jnp.broadcast_to(by_query[:, None, :], (per_device, probe_count, probe_count))
    chosen = iota((pair_count, probe_count), 1) == lax.rem(iota((pair_count, probe_count), 0), probe_count)
    pcol = jnp.sum(
        jnp.where(chosen, spread.reshape(pair_count, probe_count), 0.0), axis=1, keepdims=True
    ).astype(jnp.int32)
    owner_col = lax.div(pcol, local_count)
    hits = (owner_col == iota((pair_count, owner_count), 1)).astype(jnp.float32)
    earlier = (iota((pair_count, pair_count), 0) > iota((pair_count, pair_count), 1)).astype(jnp.float32)
    before = jnp.dot(
        earlier.astype(jnp.bfloat16), hits.astype(jnp.bfloat16), preferred_element_type=jnp.float32
    )
    rank = jnp.sum(hits * before, axis=1, keepdims=True).astype(jnp.int32)
    slot_col = owner_col * cap + rank
    slot_ref[...] = slot_col
    code_col = slot_col * local_count + lax.rem(pcol, local_count)
    lane = iota((pair_count, LANES), 1)
    at_lane = lax.rem(lane, per_device) == lax.div(iota((pair_count, LANES), 0), probe_count)
    gcode[0] = jnp.sum(jnp.where(at_lane, code_col, 0).reshape(per_device, probe_count, LANES), axis=0)

    row = iota((rows, LANES), 0)
    dest = lax.div(row, 2 * cap)
    second = shift_of(lax.div(dest, 2))
    yy = wrap(y + second * (1 - core))
    xx = wrap(x + second * core)
    row_slot = ((yy * side + xx) * 2 + lax.rem(dest, 2)) * cap + lax.rem(row, cap)
    mine = lax.rem(lax.div(row, cap), 2) == lax.div(iota((rows, LANES), 1), per_device)
    tgt[...] = jnp.where(mine, row_slot, -1)

    with jax.named_scope("load"):
        own_q.wait()
    with jax.named_scope("barrier"):
        pl.semaphore_wait(barrier, 4 * (side - 1) + 1)

    def code_to(t):
        return remote(gcode.at[0], gcode.at[t], gc_send.at[t], gc_recv.at[t], at(on_first[t] + core))

    half = per_device // 2

    def along(distance):
        return at(on_first[number_of(distance, side)] + core)

    def hop(t):
        if t < 5:
            return [remote(gq.at[0], gq.at[t], gq_send.at[t], gq_recv.at[t], along(shift_int(t)))]
        if t < side - 1:
            return [remote(gq.at[t - 2], gq.at[t], gq_send.at[t], gq_recv.at[t], along(1 if t % 2 else -1))]
        parts = []
        for n, (src, step) in enumerate(((t - 4, 2), (t - 3, -2))):
            here = pl.ds(n * half, half)
            parts.append(remote(gq.at[src, here], gq.at[t, here], gq_send.at[t + n], gq_recv.at[t], along(step)))
        return parts

    for t in (1, 2, 3, 4):
        for copy in hop(t):
            copy.start()
    for t in range(1, side):
        code_to(t).start()
    def to_owner(p, f, dest_core):
        dev = at(on_second[f] + dest_core)
        d = f * 2 + dest_core
        return (
            remote(snd.at[p, d], rcv.at[p, f * 2 + core], x_send.at[p], x_recv.at[p], dev),
            remote(scid.at[p, d], rcid.at[p, f * 2 + core], c_send.at[p], c_recv.at[p], dev),
        )

    def whole(ref, sem):
        return pltpu.make_async_copy(ref, ref, sem)

    def come(t):
        whole(gq.at[t], gq_recv.at[t]).wait()
        if t == 3:
            hop(5)[0].start()
            hop(7)[0].start()
        if t == 4:
            hop(6)[0].start()
            hop(7)[1].start()

    def arrived(p):
        for t in ((), (1,), (2, 3, 4), (5,), (6, 7))[p + 1]:
            come(t)
        for t in (2 * p, 2 * p + 1):
            if t:
                code_to(t).wait_recv()

    def build(p):
        code = jnp.where(iota((probe_count, LANES), 1) < per_device, gcode[2 * p], gcode[2 * p + 1])
        slot_of = lax.div(code, local_count)
        mark_of = (lax.rem(code, local_count) + 1).astype(jnp.float32)
        target = tgt[...]
        mark = jnp.zeros((rows, LANES), jnp.float32)
        for j in range(probe_count):
            mark = jnp.where(target == slot_of[j : j + 1, :], mark_of[j : j + 1, :], mark)
        pick = jnp.where(mark > 0.0, 1.0, 0.0).astype(jnp.bfloat16)
        step = 256
        for n in range(0, width, step):
            part = gq[2 * p : 2 * p + 2, :, n : n + step].reshape(2 * per_device, step)
            took = jnp.dot(pick, part, preferred_element_type=jnp.float32)
            snd[p, :, :, n : n + step] = took.astype(jnp.bfloat16).reshape(dests, 2 * cap, step)
        mark_col = jnp.sum(mark, axis=1, keepdims=True)
        spot = iota((rows, LANES), 1) == lax.rem(iota((rows, LANES), 0), 2 * cap)
        marks = jnp.sum(jnp.where(spot, mark_col, 0.0).reshape(dests, 2 * cap, LANES), axis=1)
        for d in range(dests):
            scid[p, d] = marks[d : d + 1, :]

    def send(p):
        self_x = pltpu.make_async_copy(snd.at[p, core], rcv.at[p, core], x_recv.at[p])
        self_c = pltpu.make_async_copy(scid.at[p, core], rcid.at[p, core], c_recv.at[p])
        self_c.start()
        self_x.start()
        for f in range(side - 1, 0, -1):
            for dest_core in range(2):
                for copy in to_owner(p, f, dest_core):
                    copy.start()
        for copy in to_owner(p, 0, 1 - core):
            copy.start()

    def back(p, f, cls, i):
        t = 2 * p + i
        a, b = mirror[t], mirror[f]
        if f + t:
            dev = at((ys[a] + xs[b] if cls else ys[b] + xs[a]) + cls)
        else:
            dev = at(partner)
        b = (f * 2 + cls) * 2 + i
        land = (f * 2 + core) * 2 + i
        return (
            remote(sm.at[p, b], rmeta.at[p, land], m_send.at[p], m_recv.at[p], dev),
            remote(rs.at[p, b], ret.at[p, land], b_send.at[p], b_recv.at[p], dev),
        )

    def score(p):
        row = iota((rows, LANES), 0)
        lane = iota((rows, LANES), 1)
        seen = jnp.broadcast_to(rcid[p], (dests, 2 * cap, LANES)).reshape(rows, LANES)
        cid = jnp.sum(jnp.where(lane == lax.rem(row, 2 * cap), seen, 0.0), axis=1, keepdims=True) - 1.0
        cid = cid.astype(jnp.int32)
        acc[...] = jnp.zeros_like(acc)

        def cluster(c, carry):
            got = lax.dot_general(
                rcv[p].reshape(rows, width),
                pv[c],
                (((1,), (1,)), ((), ())),
                preferred_element_type=jnp.float32,
            )
            acc[...] = jnp.where(cid == c, got, acc[...])
            return carry

        lax.fori_loop(0, local_count, cluster, 0, unroll=8)
        centres = lax.dot_general(
            rcv[p].reshape(rows, width),
            cent_ref[...],
            (((1,), (1,)), ((), ())),
            preferred_element_type=jnp.float32,
        )
        of_row = iota((rows, local_count), 1) == cid
        centre = jnp.sum(jnp.where(of_row, centres, 0.0), axis=1, keepdims=True)
        live = jnp.sum(jnp.where(of_row, cnt_ref[...].astype(jnp.float32), 0.0), axis=1, keepdims=True)
        within = iota((rows, span), 1).astype(jnp.float32) < live
        value = jnp.where(within, acc[...] + centre, 0.0)
        top = jnp.maximum(jnp.max(jnp.abs(value), axis=1, keepdims=True), 1e-30)
        coded = jnp.round(value * (CODE_TOP / top)).astype(jnp.int32)
        low, high = coded[:, : span // 2], coded[:, span // 2 :]
        rs[p] = (high * 65536 + (low & 65535)).reshape(dests * 2, cap, LANES)
        spot = lax.rem(lane, cap) == lax.rem(row, cap)
        even = lax.rem(lax.div(lane, cap), 2) == 0
        both = jnp.where(even, top * (1.0 / CODE_TOP), live)
        both = jnp.sum(jnp.where(spot, both, 0.0).reshape(dests * 2, cap, LANES), axis=1)
        for b in range(dests * 2):
            sm[p, b] = both[b : b + 1, :]

    def give_all(p):
        for f in range(side - 1, -1, -1):
            for i in (1, 0):
                for cls in range(2):
                    if f + p + i:
                        for copy in back(p, f, cls, i):
                            copy.start()
        if p == 0:
            self_b = core * 2
            pltpu.make_async_copy(sm.at[0, self_b], rmeta.at[0, self_b], m_recv.at[0]).start()
            pltpu.make_async_copy(rs.at[0, self_b], ret.at[0, self_b], b_recv.at[0]).start()
            for copy in back(0, 0, 1 - core, 0):
                copy.start()

    scale_col = jnp.zeros((pair_count, 1), jnp.float32)
    live_col = jnp.zeros((pair_count, 1), jnp.float32)

    def finish(p, scale_col, live_col):
        slots = slot_ref[...]
        spot_lane = iota((1, rows), 1)
        block = lax.div(spot_lane, cap)
        second = shift_of(lax.div(block, 4))
        first = shift_of(2 * p + lax.rem(block, 2))
        yy = wrap(y + second * (1 - core) + first * core)
        xx = wrap(x + first * (1 - core) + second * core)
        have = ((yy * side + xx) * 2 + lax.rem(lax.div(block, 2), 2)) * cap + lax.rem(spot_lane, cap)
        match = slots == have
        pick = jnp.where(match, 1.0, 0.0).astype(jnp.bfloat16)
        words = ret[p].reshape(rows, LANES)

        def piece(low, high):
            return jnp.concatenate([low, high], axis=1).astype(jnp.float32).astype(jnp.bfloat16)

        tops = piece(
            lax.shift_right_arithmetic(lax.shift_left(words, 16), 24), lax.shift_right_arithmetic(words, 24)
        )
        tails = piece(words & 255, lax.shift_right_arithmetic(words, 16) & 255)
        sums = 256.0 * jnp.dot(pick, tops, preferred_element_type=jnp.float32) + jnp.dot(
            pick, tails, preferred_element_type=jnp.float32
        )
        out_ref[...] = sums if p == 0 else out_ref[...] + sums
        each = LANES // cap
        scale_lane, live_lane = [], []
        for h in range(rows // LANES):
            meta = jnp.concatenate([rmeta[p, h * each + b] for b in range(each)], axis=0)
            group, block = lax.div(iota((each, LANES), 1), cap), iota((each, LANES), 0)
            twin = block + 1 - 2 * lax.rem(block, 2)
            here = jnp.sum(jnp.where(group == block, meta, 0.0), axis=0, keepdims=True)
            there = jnp.sum(jnp.where(group == twin, meta, 0.0), axis=0, keepdims=True)
            even = lax.rem(lax.div(iota((1, LANES), 1), cap), 2) == 0
            scale_lane.append(jnp.where(even, here, pltpu.roll(there, cap, 1)))
            live_lane.append(jnp.where(even, pltpu.roll(there, LANES - cap, 1), here))
        scale_col += jnp.sum(
            jnp.where(match, jnp.concatenate(scale_lane, axis=1), 0.0), axis=1, keepdims=True
        )
        live_col += jnp.sum(jnp.where(match, jnp.concatenate(live_lane, axis=1), 0.0), axis=1, keepdims=True)
        return scale_col, live_col

    for step in ORDER:
        kind, p = step[0], int(step[1:] or 0)
        with jax.named_scope(step):
            if kind == "B":
                arrived(p)
                build(p)
                send(p)
            if kind == "P":
                own_p.start()
            if kind == "X":
                whole(rcid.at[p], c_recv.at[p]).wait()
                whole(rcv.at[p], x_recv.at[p]).wait()
            if kind == "S":
                if p == 0:
                    own_p.wait()
                score(p)
            if kind == "G":
                give_all(p)
            if kind == "F":
                whole(rmeta.at[p], m_recv.at[p]).wait()
                whole(ret.at[p], b_recv.at[p]).wait()
                scale_col, live_col = finish(p, scale_col, live_col)

    out_ref[...] = out_ref[...] * scale_col
    at_query = iota((pair_count, per_device), 1) == lax.div(iota((pair_count, per_device), 0), probe_count)
    vis_ref[...] = jnp.sum(jnp.where(at_query, live_col, 0.0), axis=0, keepdims=True).astype(jnp.int32)

    for t in range(1, side):
        code_to(t).wait_send()
        for copy in hop(t):
            copy.wait_send()
    for p in range(pairs):
        whole(snd.at[p, pl.ds(0, dests - 1)], x_send.at[p]).wait()
        whole(scid.at[p, pl.ds(0, dests - 1)], c_send.at[p]).wait()
        blocks = dests * 2 - (1 if p == 0 else 0)
        whole(rs.at[p, pl.ds(0, blocks)], b_send.at[p]).wait()
        whole(sm.at[p, pl.ds(0, blocks)], m_send.at[p]).wait()


def body(queries, probes, passages, centroids, counts):
    owner_count = lax.axis_size("owner")
    side = math.isqrt(owner_count // 2)
    per_device, probe_count = probes.shape
    local_count, span, width = passages.shape
    pair_count = per_device * probe_count
    cap = 2 * pair_count // owner_count
    pairs = side // 2
    dests = side * 2
    rows = dests * 2 * cap
    vmem = pl.BlockSpec(memory_space=pltpu.VMEM)
    hbm = pl.BlockSpec(memory_space=pltpu.HBM)
    dma = pltpu.SemaphoreType.DMA
    scores, visits = pl.pallas_call(
        functools.partial(kernel, side, cap),
        out_shape=(
            jax.ShapeDtypeStruct((pair_count, span), jnp.float32),
            jax.ShapeDtypeStruct((1, per_device), jnp.int32),
        ),
        in_specs=[hbm] * 5,
        out_specs=(vmem, vmem),
        scratch_shapes=[
            pltpu.VMEM((probe_count, per_device), jnp.int32),
            pltpu.VMEM((local_count, width), jnp.bfloat16),
            pltpu.VMEM((1, local_count), jnp.int32),
            pltpu.VMEM((side, per_device, width), jnp.bfloat16),
            pltpu.VMEM((side, probe_count, LANES), jnp.int32),
            pltpu.VMEM((pairs, dests, 2 * cap, width), jnp.bfloat16),
            pltpu.VMEM((pairs, dests, 1, LANES), jnp.float32),
            pltpu.VMEM((pairs, dests, 2 * cap, width), jnp.bfloat16),
            pltpu.VMEM((pairs, dests, 1, LANES), jnp.float32),
            pltpu.VMEM((rows, span), jnp.float32),
            pltpu.VMEM((pairs, dests * 2, cap, LANES), jnp.int32),
            pltpu.VMEM((pairs, dests * 2, 1, LANES), jnp.float32),
            pltpu.VMEM((pairs, dests * 2, cap, LANES), jnp.int32),
            pltpu.VMEM((pairs, dests * 2, 1, LANES), jnp.float32),
            pltpu.VMEM((local_count, span, width), jnp.bfloat16),
            pltpu.VMEM((rows, LANES), jnp.int32),
            pltpu.VMEM((pair_count, 1), jnp.int32),
            dma,
            dma((3,)),
            dma,
            dma((side + 1,)),
            dma((side,)),
            dma((side,)),
            dma((side,)),
            dma((pairs,)),
            dma((pairs,)),
            dma((pairs,)),
            dma((pairs,)),
            dma((pairs,)),
            dma((pairs,)),
            dma((pairs,)),
            dma((pairs,)),
        ],
        compiler_params=pltpu.CompilerParams(
            collective_id=0, has_side_effects=True, vmem_limit_bytes=60 * 1024 * 1024
        ),
    )(
        queries,
        probes.T,
        passages,
        centroids,
        counts.reshape(1, local_count),
    )
    return scores.reshape(per_device, probe_count, span), visits.reshape(per_device)


def solution(mesh):
    in_specs = (
        P(("groups", "owner"), None),
        P(("groups", "owner"), None),
        P("owner", None, None),
        P("owner", None),
        P("owner"),
    )
    out_specs = (P(("groups", "owner"), None, None), P(("groups", "owner")))
    return jax.shard_map(body, mesh=mesh, in_specs=in_specs, out_specs=out_specs, check_vma=False)
```

```python
import functools
import math

import jax
import jax.numpy as jnp
from jax import lax
from jax.experimental import pallas as pl
from jax.experimental.pallas import tpu as pltpu
from jax.sharding import PartitionSpec as P

MESH = pl.DeviceIdType.MESH
LANES = 128
CODE_TOP = 32767.0
LEVELS, LEVEL_BASE, COUNT_BASE = 32.0, 8192.0, 512.0
ORDER = (
    "B0", "P", "B1", "T0", "T1", "B2", "T2", "T3", "X0", "S0", "B3", "X1", "S1", "G0",
    "X2", "S2", "G1", "X30", "G2", "S30", "G30", "X31", "S31", "G31", "F0", "F1", "F2", "F3",
)


def iota(shape, dim):
    return lax.broadcasted_iota(jnp.int32, shape, dim)


def shift_of(t):
    return (2 * lax.rem(t, 2) - 1) * lax.div(t + 1, 2)


def shift_int(t):
    return (t + 1) // 2 * (1 if t % 2 else -1)


def number_of(shift, side):
    return next(t for t in range(side) if (shift_int(t) - shift) % side == 0)


def kernel(
    side,
    cap,
    q_hbm,
    probe_hbm,
    pass_hbm,
    cent_hbm,
    cnt_hbm,
    out_ref,
    vis_ref,
    probe_ref,
    cent_ref,
    cnt_ref,
    gq,
    gcode,
    snd,
    scid,
    rcv,
    rcid,
    acc,
    rs,
    ret,
    pv,
    pvt,
    tgt,
    slot_ref,
    load_sem,
    small_sem,
    pass_sem,
    gq_send,
    gq_recv,
    gc_send,
    gc_recv,
    x_send,
    x_recv,
    c_send,
    c_recv,
    b_send,
    b_recv,
):
    me = lax.axis_index("owner")
    core = lax.rem(me, 2)
    x = lax.rem(lax.div(me, 2), side)
    y = lax.div(me, 2 * side)
    local_count, span, width = pv.shape
    per_device = gq.shape[1]
    probe_count = probe_ref.shape[0]
    pair_count = per_device * probe_count
    owner_count = side * side * 2
    pairs = side // 2
    dests = side * 2
    rows = dests * 2 * cap

    def wrap(v):
        return lax.rem(v + side, side)

    ys = [wrap(y + shift_int(t)) * (2 * side) for t in range(side)]
    xs = [wrap(x + shift_int(t)) * 2 for t in range(side)]
    on_first = [(1 - core) * (ys[0] + xs[t]) + core * (ys[t] + xs[0]) for t in range(side)]
    on_second = [(1 - core) * (ys[t] + xs[0]) + core * (ys[0] + xs[t]) for t in range(side)]
    mirror = [number_of(-shift_int(t), side) for t in range(side)]

    def at(index):
        return {"owner": index}

    def remote(src, dst, send, recv, dev):
        return pltpu.make_async_remote_copy(
            src_ref=src, dst_ref=dst, send_sem=send, recv_sem=recv, device_id=dev, device_id_type=MESH
        )

    small = [
        pltpu.make_async_copy(src, dst, small_sem.at[n])
        for n, (src, dst) in enumerate(((probe_hbm, probe_ref), (cent_hbm, cent_ref), (cnt_hbm, cnt_ref)))
    ]
    for copy in small:
        copy.start()
    own_q = pltpu.make_async_copy(q_hbm, gq.at[0], load_sem)
    own_q.start()
    own_p = pltpu.make_async_copy(pass_hbm, pv, pass_sem)

    barrier = pltpu.get_barrier_semaphore()

    for t in range(1, side):
        for dest_core in range(2):
            for index in (ys[t] + xs[0], ys[0] + xs[t]):
                pl.semaphore_signal(barrier, inc=1, device_id=at(index + dest_core), device_id_type=MESH)
    partner = ys[0] + xs[0] + 1 - core
    pl.semaphore_signal(barrier, inc=1, device_id=at(partner), device_id_type=MESH)

    for copy in small:
        copy.wait()
    by_query = jnp.transpose(probe_ref[...].astype(jnp.float32))
    spread = jnp.broadcast_to(by_query[:, None, :], (per_device, probe_count, probe_count))
    chosen = iota((pair_count, probe_count), 1) == lax.rem(iota((pair_count, probe_count), 0), probe_count)
    pcol = jnp.sum(
        jnp.where(chosen, spread.reshape(pair_count, probe_count), 0.0), axis=1, keepdims=True
    ).astype(jnp.int32)
    owner_col = lax.div(pcol, local_count)
    hits = (owner_col == iota((pair_count, owner_count), 1)).astype(jnp.float32)
    earlier = (iota((pair_count, pair_count), 0) > iota((pair_count, pair_count), 1)).astype(jnp.float32)
    before = jnp.dot(
        earlier.astype(jnp.bfloat16), hits.astype(jnp.bfloat16), preferred_element_type=jnp.float32
    )
    rank = jnp.sum(hits * before, axis=1, keepdims=True).astype(jnp.int32)
    slot_col = owner_col * cap + rank
    slot_ref[...] = slot_col
    code_col = slot_col * local_count + lax.rem(pcol, local_count)
    lane = iota((pair_count, LANES), 1)
    at_lane = lax.rem(lane, per_device) == lax.div(iota((pair_count, LANES), 0), probe_count)
    gcode[0] = jnp.sum(jnp.where(at_lane, code_col, 0).reshape(per_device, probe_count, LANES), axis=0)

    row = iota((rows, LANES), 0)
    dest = lax.div(row, 2 * cap)
    second = shift_of(lax.div(dest, 2))
    yy = wrap(y + second * (1 - core))
    xx = wrap(x + second * core)
    row_slot = ((yy * side + xx) * 2 + lax.rem(dest, 2)) * cap + lax.rem(row, cap)
    mine = lax.rem(lax.div(row, cap), 2) == lax.div(iota((rows, LANES), 1), per_device)
    tgt[...] = jnp.where(mine, row_slot, -1)

    with jax.named_scope("load"):
        own_q.wait()
    with jax.named_scope("barrier"):
        pl.semaphore_wait(barrier, 4 * (side - 1) + 1)

    def code_to(t):
        return remote(gcode.at[0], gcode.at[t], gc_send.at[t], gc_recv.at[t], at(on_first[t] + core))

    half = per_device // 2

    def along(distance):
        return at(on_first[number_of(distance, side)] + core)

    def hop(t):
        if t < 5:
            return [remote(gq.at[0], gq.at[t], gq_send.at[t], gq_recv.at[t], along(shift_int(t)))]
        if t < side - 1:
            return [remote(gq.at[t - 2], gq.at[t], gq_send.at[t], gq_recv.at[t], along(1 if t % 2 else -1))]
        parts = []
        for n, (src, step) in enumerate(((t - 4, 2), (t - 3, -2))):
            here = pl.ds(n * half, half)
            parts.append(remote(gq.at[src, here], gq.at[t, here], gq_send.at[t + n], gq_recv.at[t], along(step)))
        return parts

    for t in (1, 2, 3, 4):
        for copy in hop(t):
            copy.start()
    for t in range(1, side):
        code_to(t).start()
    def to_owner(p, f, dest_core):
        dev = at(on_second[f] + dest_core)
        d = f * 2 + dest_core
        return (
            remote(snd.at[p, d], rcv.at[p, f * 2 + core], x_send.at[p], x_recv.at[p, f // (side // 2)], dev),
            remote(scid.at[p, d], rcid.at[p, f * 2 + core], c_send.at[p], c_recv.at[p, f // (side // 2)], dev),
        )

    def whole(ref, sem):
        return pltpu.make_async_copy(ref, ref, sem)

    def come(t):
        whole(gq.at[t], gq_recv.at[t]).wait()
        if t == 3:
            hop(5)[0].start()
            hop(7)[0].start()
        if t == 4:
            hop(6)[0].start()
            hop(7)[1].start()

    def arrived(p):
        for t in ((), (1,), (2, 3, 4), (5,), (6, 7))[p + 1]:
            come(t)
        for t in (2 * p, 2 * p + 1):
            if t:
                code_to(t).wait_recv()

    def build(p):
        code = jnp.where(iota((probe_count, LANES), 1) < per_device, gcode[2 * p], gcode[2 * p + 1])
        slot_of = lax.div(code, local_count)
        mark_of = (lax.rem(code, local_count) + 1).astype(jnp.float32)
        target = tgt[...]
        mark = jnp.zeros((rows, LANES), jnp.float32)
        for j in range(probe_count):
            mark = jnp.where(target == slot_of[j : j + 1, :], mark_of[j : j + 1, :], mark)
        pick = jnp.where(mark > 0.0, 1.0, 0.0).astype(jnp.bfloat16)
        step = 256
        for n in range(0, width, step):
            part = gq[2 * p : 2 * p + 2, :, n : n + step].reshape(2 * per_device, step)
            took = jnp.dot(pick, part, preferred_element_type=jnp.float32)
            snd[p, :, :, n : n + step] = took.astype(jnp.bfloat16).reshape(dests, 2 * cap, step)
        mark_col = jnp.sum(mark, axis=1, keepdims=True)
        spot = iota((rows, LANES), 1) == lax.rem(iota((rows, LANES), 0), 2 * cap)
        marks = jnp.sum(jnp.where(spot, mark_col, 0.0).reshape(dests, 2 * cap, LANES), axis=1)
        for d in range(dests):
            scid[p, d] = marks[d : d + 1, :]

    def send(p):
        self_x = pltpu.make_async_copy(snd.at[p, core], rcv.at[p, core], x_recv.at[p, 0])
        self_c = pltpu.make_async_copy(scid.at[p, core], rcid.at[p, core], c_recv.at[p, 0])
        self_c.start()
        self_x.start()
        for f in range(side - 1, 0, -1):
            for dest_core in range(2):
                for copy in to_owner(p, f, dest_core):
                    copy.start()
        for copy in to_owner(p, 0, 1 - core):
            copy.start()

    used = pl.ds(0, cap + 1)

    def back(p, f, cls, i):
        t = 2 * p + i
        a, b = mirror[t], mirror[f]
        if f + t:
            dev = at((ys[a] + xs[b] if cls else ys[b] + xs[a]) + cls)
        else:
            dev = at(partner)
        b = (f * 2 + cls) * 2 + i
        land = (f * 2 + core) * 2 + i
        return remote(rs.at[p, b, used], ret.at[p, land, used], b_send.at[p], b_recv.at[p], dev)

    def score(p, first, count):
        rows = count * 2 * cap
        part = pl.ds(first, count)
        sums = acc.at[pl.ds(0, rows)]
        row = iota((rows, LANES), 0)
        lane = iota((rows, LANES), 1)
        seen = jnp.broadcast_to(rcid[p, part], (count, 2 * cap, LANES)).reshape(rows, LANES)
        cid = jnp.sum(jnp.where(lane == lax.rem(row, 2 * cap), seen, 0.0), axis=1, keepdims=True) - 1.0
        cid = cid.astype(jnp.int32)
        sums[...] = jnp.zeros_like(sums)

        def cluster(c, carry):
            got = jnp.dot(
                rcv[p, part].reshape(rows, width), pvt[c], preferred_element_type=jnp.float32
            )
            sums[...] = jnp.where(cid == c, got, sums[...])
            return carry

        lax.fori_loop(0, local_count, cluster, 0, unroll=8)
        centres = lax.dot_general(
            rcv[p, part].reshape(rows, width),
            cent_ref[...],
            (((1,), (1,)), ((), ())),
            preferred_element_type=jnp.float32,
        )
        of_row = iota((rows, local_count), 1) == cid
        centre = jnp.sum(jnp.where(of_row, centres, 0.0), axis=1, keepdims=True)
        live = jnp.sum(jnp.where(of_row, cnt_ref[...].astype(jnp.float32), 0.0), axis=1, keepdims=True)
        within = iota((rows, span), 1).astype(jnp.float32) < live
        value = jnp.where(within, sums[...] + centre, 0.0)
        top = jnp.maximum(jnp.max(jnp.abs(value), axis=1, keepdims=True), 1e-30)
        level = jnp.ceil(jnp.log2(top) * LEVELS)
        coded = jnp.round(value * (CODE_TOP / jnp.exp2(level * (1.0 / LEVELS)))).astype(jnp.int32)
        low, high = coded[:, : span // 2], coded[:, span // 2 :]
        words = (high * 65536 + (low & 65535)).reshape(count * 2, cap, LANES)
        rs[p, pl.ds(first * 2, count * 2), pl.ds(0, cap)] = words
        spot = lax.rem(lane, cap) == lax.rem(row, cap)
        both = (level + LEVEL_BASE) * COUNT_BASE + live
        both = jnp.sum(jnp.where(spot, both, 0.0).reshape(count * 2, cap, LANES), axis=1).astype(jnp.int32)
        for b in range(count * 2):
            rs[p, first * 2 + b, pl.ds(cap, 1)] = both[b : b + 1, :]

    def give_all(p, peers):
        for f in peers:
            for i in (1, 0):
                for cls in range(2):
                    if f + p + i:
                        back(p, f, cls, i).start()
        if p == 0:
            self_b = core * 2
            pltpu.make_async_copy(rs.at[0, self_b, used], ret.at[0, self_b, used], b_recv.at[0]).start()
            back(0, 0, 1 - core, 0).start()

    both_col = jnp.zeros((pair_count, 1), jnp.float32)

    def finish(p, both_col):
        slots = slot_ref[...]
        spot_lane = iota((1, rows), 1)
        block = lax.div(spot_lane, cap)
        second = shift_of(lax.div(block, 4))
        first = shift_of(2 * p + lax.rem(block, 2))
        yy = wrap(y + second * (1 - core) + first * core)
        xx = wrap(x + first * (1 - core) + second * core)
        have = ((yy * side + xx) * 2 + lax.rem(lax.div(block, 2), 2)) * cap + lax.rem(spot_lane, cap)
        match = slots == have
        pick = jnp.where(match, 1.0, 0.0).astype(jnp.bfloat16)
        words = ret[p, :, pl.ds(0, cap)].reshape(rows, LANES)

        def piece(low, high):
            return jnp.concatenate([low, high], axis=1).astype(jnp.float32).astype(jnp.bfloat16)

        tops = piece(
            lax.shift_right_arithmetic(lax.shift_left(words, 16), 24), lax.shift_right_arithmetic(words, 24)
        )
        tails = piece(words & 255, lax.shift_right_arithmetic(words, 16) & 255)
        sums = 256.0 * jnp.dot(pick, tops, preferred_element_type=jnp.float32) + jnp.dot(
            pick, tails, preferred_element_type=jnp.float32
        )
        out_ref[...] = sums if p == 0 else out_ref[...] + sums
        each = LANES // cap
        both_lane = []
        for h in range(rows // LANES):
            meta = jnp.concatenate([ret[p, h * each + b, pl.ds(cap, 1)] for b in range(each)], axis=0)
            keep = lax.div(iota((each, LANES), 1), cap) == iota((each, LANES), 0)
            both_lane.append(jnp.sum(jnp.where(keep, meta.astype(jnp.float32), 0.0), axis=0, keepdims=True))
        return both_col + jnp.sum(
            jnp.where(match, jnp.concatenate(both_lane, axis=1), 0.0), axis=1, keepdims=True
        )

    quarter = local_count // 4

    def turn(n):
        def one(c, carry):
            pvt[c] = jnp.transpose(pv[c])
            return carry

        lax.fori_loop(n * quarter, (n + 1) * quarter, one, 0)

    for step in ORDER:
        kind, p = step[0], int(step[1:2] or 0)
        halves = (int(step[2:]),) if step[2:] else (0, 1)
        peers = range(halves[0] * (side // 2), (halves[-1] + 1) * (side // 2))
        with jax.named_scope(step):
            if kind == "B":
                arrived(p)
                build(p)
                send(p)
            if kind == "P":
                own_p.start()
            if kind == "T":
                if p == 0:
                    own_p.wait()
                turn(p)
            if kind == "X":
                for h in halves:
                    here = pl.ds(h * side, side)
                    whole(rcid.at[p, here], c_recv.at[p, h]).wait()
                    whole(rcv.at[p, here], x_recv.at[p, h]).wait()
            if kind == "S":
                score(p, halves[0] * side, len(halves) * side)
            if kind == "G":
                give_all(p, peers)
            if kind == "F":
                whole(ret.at[p, :, used], b_recv.at[p]).wait()
                both_col = finish(p, both_col)

    level_col = jnp.floor(both_col * (1.0 / COUNT_BASE))
    live_col = both_col - level_col * COUNT_BASE
    out_ref[...] = out_ref[...] * (jnp.exp2((level_col - LEVEL_BASE) * (1.0 / LEVELS)) * (1.0 / CODE_TOP))
    at_query = iota((pair_count, per_device), 1) == lax.div(iota((pair_count, per_device), 0), probe_count)
    vis_ref[...] = jnp.sum(jnp.where(at_query, live_col, 0.0), axis=0, keepdims=True).astype(jnp.int32)

    for t in range(1, side):
        code_to(t).wait_send()
        for copy in hop(t):
            copy.wait_send()
    for p in range(pairs):
        whole(snd.at[p, pl.ds(0, dests - 1)], x_send.at[p]).wait()
        whole(scid.at[p, pl.ds(0, dests - 1)], c_send.at[p]).wait()
        blocks = dests * 2 - (1 if p == 0 else 0)
        whole(rs.at[p, pl.ds(0, blocks), used], b_send.at[p]).wait()


def body(queries, probes, passages, centroids, counts):
    owner_count = lax.axis_size("owner")
    side = math.isqrt(owner_count // 2)
    per_device, probe_count = probes.shape
    local_count, span, width = passages.shape
    pair_count = per_device * probe_count
    cap = 2 * pair_count // owner_count
    pairs = side // 2
    dests = side * 2
    rows = dests * 2 * cap
    vmem = pl.BlockSpec(memory_space=pltpu.VMEM)
    hbm = pl.BlockSpec(memory_space=pltpu.HBM)
    dma = pltpu.SemaphoreType.DMA
    scores, visits = pl.pallas_call(
        functools.partial(kernel, side, cap),
        out_shape=(
            jax.ShapeDtypeStruct((pair_count, span), jnp.float32),
            jax.ShapeDtypeStruct((1, per_device), jnp.int32),
        ),
        in_specs=[hbm] * 5,
        out_specs=(vmem, vmem),
        scratch_shapes=[
            pltpu.VMEM((probe_count, per_device), jnp.int32),
            pltpu.VMEM((local_count, width), jnp.bfloat16),
            pltpu.VMEM((1, local_count), jnp.int32),
            pltpu.VMEM((side, per_device, width), jnp.bfloat16),
            pltpu.VMEM((side, probe_count, LANES), jnp.int32),
            pltpu.VMEM((pairs, dests, 2 * cap, width), jnp.bfloat16),
            pltpu.VMEM((pairs, dests, 1, LANES), jnp.float32),
            pltpu.VMEM((pairs, dests, 2 * cap, width), jnp.bfloat16),
            pltpu.VMEM((pairs, dests, 1, LANES), jnp.float32),
            pltpu.VMEM((rows, span), jnp.float32),
            pltpu.VMEM((pairs, dests * 2, 2 * cap, LANES), jnp.int32),
            pltpu.VMEM((pairs, dests * 2, 2 * cap, LANES), jnp.int32),
            pltpu.VMEM((local_count, span, width), jnp.bfloat16),
            pltpu.VMEM((local_count, width, span), jnp.bfloat16),
            pltpu.VMEM((rows, LANES), jnp.int32),
            pltpu.VMEM((pair_count, 1), jnp.int32),
            dma,
            dma((3,)),
            dma,
            dma((side + 1,)),
            dma((side,)),
            dma((side,)),
            dma((side,)),
            dma((pairs,)),
            dma((pairs, 2)),
            dma((pairs,)),
            dma((pairs, 2)),
            dma((pairs,)),
            dma((pairs,)),
        ],
        compiler_params=pltpu.CompilerParams(
            collective_id=0, has_side_effects=True, vmem_limit_bytes=60 * 1024 * 1024
        ),
    )(
        queries,
        probes.T,
        passages,
        centroids,
        counts.reshape(1, local_count),
    )
    return scores.reshape(per_device, probe_count, span), visits.reshape(per_device)


def solution(mesh):
    in_specs = (
        P(("groups", "owner"), None),
        P(("groups", "owner"), None),
        P("owner", None, None),
        P("owner", None),
        P("owner"),
    )
    out_specs = (P(("groups", "owner"), None, None), P(("groups", "owner")))
    return jax.shard_map(body, mesh=mesh, in_specs=in_specs, out_specs=out_specs, check_vma=False)
```
